32 devices in a mesh: grid: 16 (over z, x, core), member: 2 (over y).
Axes of the slice: x: 2, y: 2, z: 4, core: 2. Of those that a mesh axis runs over, the one named last changes fastest.
Arguments:
- fields: bfloat16 [2, 16384, 1024], P('member', 'grid'), may hold values from -0.796875 to 0.796875
- observed: bfloat16 [100, 16384], P(None, 'grid'), may hold values from -6 to 6
- lat_weight: float32 [16384], P('grid'), may hold values from 0.3 to 6, as said below
- var_weight: float32 [100], replicated, may hold values from 0.25 to 4
- weight: bfloat16 [100, 1024], replicated, may hold values from -0.1875 to 0.1875
- bias: float32 [100], replicated, may hold values from -1 to 1
- gain: float32 [1024], replicated, may hold values from 0.1 to 1.9
Outputs:
- grad_fields: bfloat16 [2, 16384, 1024], P('member', 'grid')
- grad_weight: float32 [100, 1024], replicated
- grad_gain: float32 [1024], replicated
- grad_bias: float32 [100], replicated
- loss: float32 [], replicated
The draws below stay inside these ranges and needn't reach their ends.
Inputs may be any that keep to these rules, and one draw needn't show every extreme that they name: `lat_weight`: positive.
All inputs are finite; a program needn't handle non-finite values.
Results may differ from the reference program's by a relative error of at most 0.0014.
The reference program's roundings to bfloat16 on the way (of `normed` and `grad_pred`) count: a program that leaves them out, or rounds other values in their place, can miss the bound.
Values sent between devices are 32-bit elements; how exact they have to be, the bound alone decides.
A program may use at most 64 MiB of HBM per device.

```python
import math
import jax
import jax.numpy as jnp
from jax import lax

D = 1024
VARS = 100
MEMBERS = 2
POINTS = 16384


def draw_lat_weight(key, part):
    inner = jax.random.fold_in(key, 17)
    places = jnp.arange(POINTS).astype(jnp.float32)
    profile = 1.0 + 3.0 * places / POINTS
    factors = jax.random.uniform(inner, (POINTS,), jnp.float32, 0.5, 1.5)
    return (profile * factors).astype(jnp.float32)


def steps_of(key, shape, shards, smallest, high):
    level, own = 1.0, jax.random.fold_in(key, 6)
    for position, shards_of in shards:
        heights = jnp.exp(jax.random.uniform(jax.random.fold_in(own, position), (shards_of,), jnp.float32, smallest / len(shards), high / len(shards)))
        level = level * jnp.repeat(heights, shape[position] // shards_of).reshape([-1 if axis == position else 1 for axis in range(len(shape))])
    return level


def bell_draw(key, extent, width, most, pieces=(), kind=jnp.bfloat16):
    factor_of = steps_of(key, extent, pieces, -0.22, 0.18) if pieces else 1.0
    entries = jax.random.normal(key, extent, jnp.float32) * width * factor_of
    return jnp.minimum(jnp.maximum(entries, -most), most).astype(kind)


def setup_inputs(seed: int = 0) -> dict:
    streams_of = jax.random.split(jax.random.key(seed), 8)
    fields = bell_draw(streams_of[0], (MEMBERS, POINTS, D), 0.1, 0.796875, ((0, 2), (1, 16)))
    observed = bell_draw(streams_of[1], (VARS, POINTS), 1.0, 6.0, ((1, 16),))
    lat_weight = draw_lat_weight(jax.random.fold_in(streams_of[7], 71), 0)
    var_weight = jnp.clip(jnp.exp(jax.random.uniform(streams_of[3], (VARS,), jnp.float32, math.log(0.25), math.log(4.0))), 0.25, 4.0)
    weight = bell_draw(streams_of[4], (VARS, D), D ** -0.5, 0.1875)
    bias = jnp.clip(jax.random.uniform(streams_of[5], (VARS,), jnp.float32, -1.0, 1.0), -1.0, 1.0)
    gain = jnp.clip(1.0 + 0.18 * jax.random.normal(streams_of[6], (D,), jnp.float32), 0.1, 1.9)
    return dict(fields=fields, observed=observed, lat_weight=lat_weight, var_weight=var_weight, weight=weight, bias=bias, gain=gain)


soft_square = 0.01
norm_epsilon = 1e-05

def normalize(member_rows, gain):
    values = member_rows.astype(jnp.float32)
    row_mean = lax.optimization_barrier(jnp.mean(values, axis=-1, keepdims=True))
    centred = values - row_mean
    inv_std = lax.rsqrt(lax.optimization_barrier(jnp.mean(centred * centred, axis=-1, keepdims=True)) + norm_epsilon)
    unit_rows = centred * inv_std
    normed = (unit_rows * gain[None, :]).astype(jnp.bfloat16)
    return (normed, unit_rows, inv_std)

def reference(fields, observed, lat_weight, var_weight, weight, bias, gain):
    members = fields.shape[0]

    def forward(member_rows):
        normed, unit_rows, inv_std = normalize(member_rows, gain)
        return jnp.dot(weight, normed.T, preferred_element_type=jnp.float32) + bias[:, None]
    predicted = lax.map(forward, fields)
    target = observed.astype(jnp.float32)
    obs_gap = predicted - target[None]
    obs_abs = jnp.sqrt(obs_gap * obs_gap + soft_square)
    obs_sign = obs_gap / obs_abs
    sign_rows = [jnp.zeros(target.shape, jnp.float32) for member in range(members)]
    pair_abs = jnp.zeros(target.shape, jnp.float32)
    for first in range(members):
        for second in range(first + 1, members):
            gap = predicted[first] - predicted[second]
            soft_abs = jnp.sqrt(gap * gap + soft_square)
            pair_abs = pair_abs + soft_abs
            sign_rows[first] = sign_rows[first] + gap / soft_abs
            sign_rows[second] = sign_rows[second] - gap / soft_abs
    pair_sign = jnp.stack(sign_rows)
    scale_pair = 1.0 / (members * (members - 1))
    weight_grid = var_weight[:, None] * lat_weight[None, :]
    crps = lax.optimization_barrier(jnp.sum(obs_abs, axis=0)) / members - pair_abs * scale_pair
    lat_total = jnp.sum(lat_weight)
    loss = jnp.sum(weight_grid * crps) / (VARS * lat_total)
    grad_pred = (weight_grid[None] * (obs_sign / members - pair_sign * scale_pair)).astype(jnp.bfloat16)
    factor = POINTS / lat_total

    def backward(pair):
        member_rows, member_grad = pair
        normed, unit_rows, inv_std = normalize(member_rows, gain)
        grad_normed = jnp.dot(member_grad.T, weight, preferred_element_type=jnp.float32)
        grad_unit = grad_normed * gain[None, :]
        mean_one = lax.optimization_barrier(jnp.mean(grad_unit, axis=-1, keepdims=True))
        mean_two = lax.optimization_barrier(jnp.mean(grad_unit * unit_rows, axis=-1, keepdims=True))
        grad_rows = (factor * (inv_std * (grad_unit - mean_one - unit_rows * mean_two))).astype(jnp.bfloat16)
        part_weight = jnp.dot(member_grad, normed, preferred_element_type=jnp.float32)
        part_gain = lax.optimization_barrier(jnp.sum(grad_normed * unit_rows, axis=0))
        part_bias = lax.optimization_barrier(jnp.sum(member_grad.astype(jnp.float32), axis=1))
        return (grad_rows, part_weight, part_gain, part_bias)
    grad_fields, weight_parts, gain_parts, bias_parts = lax.map(backward, (fields, grad_pred))
    grad_weight = factor * lax.optimization_barrier(jnp.sum(weight_parts, axis=0))
    grad_gain = factor * lax.optimization_barrier(jnp.sum(gain_parts, axis=0))
    grad_bias = factor * lax.optimization_barrier(jnp.sum(bias_parts, axis=0))
    return (grad_fields, grad_weight, grad_gain, grad_bias, loss)
```

```python
import functools

import jax
import jax.numpy as jnp
from jax import lax
from jax.experimental import pallas as pl
from jax.experimental.pallas import tpu as pltpu
from jax.sharding import PartitionSpec as P

soft_square = 0.01
norm_epsilon = 1e-05
LANES = 128
ROW_CHUNKS = 4
POINT_BLOCK = 128
NORM_ROWS = 64
f32 = jnp.float32
bf16 = jnp.bfloat16
MESH_ID = pl.DeviceIdType.MESH


def plan(G, M, V, D):
    K = ROW_CHUNKS
    offs = [int(V * k / K / 16 + 0.5) * 16 for k in range(K)] + [V]
    rows = [offs[k + 1] - offs[k] for k in range(K)]
    extra = -(-(rows[-1] + 2) // 8) * 8
    blocks = rows[:-1] + [extra]
    C = D // LANES
    per = G // K
    S = (M * per) // C
    assert G % K == 0 and (M * per) % C == 0 and S >= 1
    return K, offs, rows, blocks, C, per, S


def to_column(row, size):
    r = lax.broadcasted_iota(jnp.int32, (size, row.shape[1]), 0)
    c = lax.broadcasted_iota(jnp.int32, (size, row.shape[1]), 1)
    return jnp.sum(jnp.where(r == c, row, 0.0), axis=1, keepdims=True)


def body(G, M, fields, obs, lat, vw, w, bias, gain,
         gf, gw, gg, gb, loss,
         x, unit, normed, inv, outb, wp, gp, pred, others, lat_own, lat_all,
         part, rs, ag_src, ag, lossb,
         in_sem, out_sem, lat_send, lat_recv, ps_first, pr_first, ps, pr,
         rs_send, rs_recv, ag_send, ag_recv):
    V, PTS = obs.shape
    D = w.shape[1]
    VP = wp.shape[0]
    N = G * M
    K, offs, rows, blocks, C, per, S = plan(G, M, V, D)
    ends = [-(-hi // 8) * 8 for hi in offs[1:]]
    J = PTS // POINT_BLOCK
    g = lax.axis_index("grid")
    m = lax.axis_index("member")
    me = m * G + g
    my_k = lax.rem(g, K)
    my_cf = m * per + g // K
    my_c = my_cf // S

    def device(t):
        return {"grid": lax.rem(t, G), "member": t // G}

    barrier = pltpu.get_barrier_semaphore()

    @pl.loop(1, N)
    def _(i):
        pl.semaphore_signal(barrier, inc=1, device_id=device(lax.rem(me + i, N)), device_id_type=MESH_ID)

    def load(j):
        at = pl.ds(pl.multiple_of(j * POINT_BLOCK, POINT_BLOCK), POINT_BLOCK)
        return pltpu.make_async_copy(fields.at[0, at], x.at[at], in_sem.at[j])

    for j in range(J):
        load(j).start()
    wp[...] = jnp.zeros(wp.shape, bf16)
    wp[0:V, :] = w[...]
    gp[...] = jnp.zeros(gp.shape, bf16)
    lat_own[...] = jnp.full(lat_own.shape, jnp.sum(lat[...]), f32)
    bias_col = to_column(bias[...], VP)
    vw_col = to_column(vw[...], VP)
    gain_row = gain[...]
    pl.semaphore_wait(barrier, N - 1)

    def lat_copy(i):
        return pltpu.make_async_remote_copy(
            lat_own, lat_all.at[g], lat_send.at[i], lat_recv.at[g],
            device_id={"grid": lax.rem(g + i, G), "member": m}, device_id_type=MESH_ID)

    @pl.loop(1, G)
    def _(i):
        lat_copy(i).start()

    def pred_copy(i, k, at, send, recv):
        return pltpu.make_async_remote_copy(
            pred.at[offs[k]:ends[k], at], others.at[i, offs[k]:ends[k], at], send, recv,
            device_id={"grid": g, "member": lax.rem(m + i, M)}, device_id_type=MESH_ID)

    def points(j):
        return pl.ds(pl.multiple_of(j * POINT_BLOCK, POINT_BLOCK), POINT_BLOCK)

    @pl.loop(0, J)
    def _(j):
        load(j).wait()
        for b in range(POINT_BLOCK // NORM_ROWS):
            at = pl.ds(pl.multiple_of(j * POINT_BLOCK + b * NORM_ROWS, NORM_ROWS), NORM_ROWS)
            values = x[at, :].astype(f32)
            centred = values - jnp.mean(values, axis=-1, keepdims=True)
            istd = lax.rsqrt(jnp.mean(centred * centred, axis=-1, keepdims=True) + norm_epsilon)
            u = centred * istd
            unit[at, :] = u
            inv[at, :] = istd
            normed[at, :] = (u * gain_row).astype(bf16)
        p = lax.dot_general(wp[...], normed[points(j), :], (((1,), (1,)), ((), ())),
                            preferred_element_type=f32)
        pred[:, points(j)] = p + bias_col
        for i in range(1, M):
            pred_copy(i, 0, points(j), ps_first.at[i, j], pr_first.at[i, j]).start()

    whole = slice(0, PTS)
    for k in range(1, K):
        for i in range(1, M):
            pred_copy(i, k, whole, ps.at[i, k], pr.at[i, k]).start()

    lat_all[g] = lat_own[...]

    @pl.loop(1, G)
    def _(i):
        src = lax.rem(g + i, G)
        pltpu.make_async_copy(lat_own, lat_all.at[src], lat_recv.at[src]).wait()

    lat_total = jnp.sum(lat_all[...], axis=0)[0:1, 0:1]
    factor = (PTS * G) / lat_total

    scale_pair = 1.0 / (M * (M - 1))
    lossb[...] = jnp.zeros(lossb.shape, f32)
    ones = jnp.ones((8, PTS), bf16)

    def unit_device(k, c):
        cf = c * S
        return cf // per, (cf % per) * K + k

    def rs_copy(k, c):
        om, og = unit_device(k, c)
        return pltpu.make_async_remote_copy(
            part.at[k, c, 0:blocks[k]], rs.at[me, 0:blocks[k]], rs_send.at[k, c], rs_recv.at[me],
            device_id={"grid": og, "member": om}, device_id_type=MESH_ID)

    def not_mine(k, c):
        om, og = unit_device(k, c)
        return jnp.logical_or(m != om, g != og)

    for k in range(K):
        for i in range(1, M):
            if k == 0:
                for j in range(J):
                    pred_copy(i, 0, points(j), ps_first.at[i, j], pr_first.at[i, j]).wait_recv()
            else:
                pred_copy(i, k, whole, ps.at[i, k], pr.at[i, k]).wait_recv()
        lo, hi, R = offs[k], offs[k + 1], rows[k]
        own = pred[lo:hi, :]
        e = own - obs[lo:hi, :].astype(f32)
        sq = e * e + soft_square
        r = lax.rsqrt(sq)
        grad = e * r * (1.0 / M)
        crps = sq * r * (1.0 / M)
        for i in range(1, M):
            e = own - others[i, lo:hi, :]
            sq = e * e + soft_square
            r = lax.rsqrt(sq)
            grad = grad - e * r * scale_pair
            crps = crps - sq * r * (0.5 * scale_pair)
        wg = vw_col[lo:hi, :] * lat[...]
        gk = (wg * grad).astype(bf16)
        lossb[...] += jnp.sum(wg * crps, axis=0, keepdims=True)
        gp[lo:hi, :] = gk
        gwk = jnp.dot(gk, normed[...], preferred_element_type=f32)
        if k == K - 1:
            gbp = lax.dot_general(ones, gp[...], (((1,), (1,)), ((), ())), preferred_element_type=f32)
            lane = jnp.zeros((1, LANES), f32)
            for j in range(PTS // LANES):
                lane = lane + lossb[:, j * LANES:(j + 1) * LANES]
        for c in range(C):
            part[k, c, 0:R] = gwk[:, c * LANES:(c + 1) * LANES]
            if k == K - 1:
                part[k, c, R:R + 1] = gbp[0:1, :]
                part[k, c, R + 1:R + 2] = lane
                if blocks[k] > R + 2:
                    part[k, c, R + 2:blocks[k]] = jnp.zeros((blocks[k] - R - 2, LANES), f32)
        for c in range(C):
            @pl.when(not_mine(k, c))
            def _(k=k, c=c):
                rs_copy(k, c).start()

    def ag_copy(k, i):
        B = blocks[k]
        return pltpu.make_async_remote_copy(
            ag_src.at[0:B], ag.at[k, my_c, 0:B], ag_send.at[i], ag_recv.at[k, my_c],
            device_id=device(lax.rem(me + i, N)), device_id_type=MESH_ID)

    is_owner = lax.rem(my_cf, S) == 0

    def reduce_and_spread(k):
        B = blocks[k]

        @pl.when(jnp.logical_and(is_owner, my_k == k))
        def _():
            def add(i, acc):
                src = lax.rem(me + i, N)
                pltpu.make_async_copy(part.at[k, 0, 0:B], rs.at[src, 0:B], rs_recv.at[src]).wait()
                return acc + rs[src, 0:B]

            acc = lax.fori_loop(1, N, add, part[k, my_c, 0:B]) * factor
            ag_src[0:B] = acc
            ag[k, my_c, 0:B] = acc

            @pl.loop(1, N)
            def _(i):
                ag_copy(k, i).start()

    def out_copy(j):
        return pltpu.make_async_copy(outb.at[points(j)], gf.at[0, points(j)], out_sem.at[j])

    def grad_block(j):
        gn = lax.dot_general(gp[:, points(j)], wp[...], (((0,), (0,)), ((), ())),
                             preferred_element_type=f32)
        gu = gn * gain_row
        u = unit[points(j), :]
        one = jnp.mean(gu, axis=-1, keepdims=True)
        two = jnp.mean(gu * u, axis=-1, keepdims=True)
        outb[points(j), :] = ((factor * inv[points(j), :]) * (gu - one - u * two)).astype(bf16)
        out_copy(j).start()

    for k in range(K - 2):
        reduce_and_spread(k)
    pl.loop(0, J // 2)(grad_block)
    for k in range(K - 2, K):
        reduce_and_spread(k)
    pl.loop(J // 2, J)(grad_block)

    gg_sum = [jnp.zeros((1, LANES), f32) for c in range(C)]
    for k in range(K):
        lo, hi, R = offs[k], offs[k + 1], rows[k]
        for c in range(C):
            @pl.when(not_mine(k, c))
            def _(k=k, c=c):
                B = blocks[k]
                pltpu.make_async_copy(part.at[k, c, 0:B], ag.at[k, c, 0:B], ag_recv.at[k, c]).wait()
        for c in range(C):
            cols = slice(c * LANES, (c + 1) * LANES)
            blk = ag[k, c, 0:R]
            gw[lo:hi, cols] = blk
            gg_sum[c] = gg_sum[c] + jnp.sum(blk * w[lo:hi, cols].astype(f32), axis=0, keepdims=True)
    for c in range(C):
        cols = slice(c * LANES, (c + 1) * LANES)
        gg[:, cols] = gg_sum[c] / gain_row[:, cols]
    last = rows[-1]
    gb[...] = ag[K - 1, 0, last:last + 1][:, 0:V]
    total = jnp.sum(ag[K - 1, 0, last + 1:last + 2], axis=1, keepdims=True)
    loss[...] = total / (factor * V * lat_total)

    @pl.loop(1, G)
    def _(i):
        lat_copy(i).wait_send()

    for i in range(1, M):
        for j in range(J):
            pred_copy(i, 0, points(j), ps_first.at[i, j], pr_first.at[i, j]).wait_send()
        for k in range(1, K):
            pred_copy(i, k, whole, ps.at[i, k], pr.at[i, k]).wait_send()
    for k in range(K):
        for c in range(C):
            @pl.when(not_mine(k, c))
            def _(k=k, c=c):
                rs_copy(k, c).wait_send()

        @pl.when(jnp.logical_and(is_owner, my_k == k))
        def _(k=k):
            @pl.loop(1, N)
            def _(i):
                ag_copy(k, i).wait_send()

    @pl.loop(0, J)
    def _(j):
        out_copy(j).wait()


def shards(fields, observed, lat_weight, var_weight, weight, bias, gain):
    G = lax.axis_size("grid")
    M = lax.axis_size("member")
    N = G * M
    V, PTS = observed.shape
    D = weight.shape[1]
    VP = -(-V // LANES) * LANES
    assert fields.shape[0] == 1 and PTS % POINT_BLOCK == 0 and VP == LANES
    K, offs, rows, blocks, C, per, S = plan(G, M, V, D)
    B = max(blocks)
    J = PTS // POINT_BLOCK
    vmem = pl.BlockSpec(memory_space=pltpu.VMEM)
    hbm = pl.BlockSpec(memory_space=pl.ANY)
    dma = pltpu.SemaphoreType.DMA
    gf, gw, gg, gb, loss = pl.pallas_call(
        functools.partial(body, G, M),
        out_shape=(
            jax.ShapeDtypeStruct(fields.shape, bf16),
            jax.ShapeDtypeStruct((V, D), f32),
            jax.ShapeDtypeStruct((1, D), f32),
            jax.ShapeDtypeStruct((1, V), f32),
            jax.ShapeDtypeStruct((1, 1), f32),
        ),
        in_specs=[hbm] + [vmem] * 6,
        out_specs=(hbm, vmem, vmem, vmem, vmem),
        scratch_shapes=[
            pltpu.VMEM((PTS, D), bf16),
            pltpu.VMEM((PTS, D), f32),
            pltpu.VMEM((PTS, D), bf16),
            pltpu.VMEM((PTS, 1), f32),
            pltpu.VMEM((PTS, D), bf16),
            pltpu.VMEM((VP, D), bf16),
            pltpu.VMEM((VP, PTS), bf16),
            pltpu.VMEM((VP, PTS), f32),
            pltpu.VMEM((M, VP, PTS), f32),
            pltpu.VMEM((8, LANES), f32),
            pltpu.VMEM((G, 8, LANES), f32),
            pltpu.VMEM((K, C, B, LANES), f32),
            pltpu.VMEM((N, B, LANES), f32),
            pltpu.VMEM((B, LANES), f32),
            pltpu.VMEM((K, C, B, LANES), f32),
            pltpu.VMEM((1, PTS), f32),
            dma((J,)), dma((J,)), dma((G,)), dma((G,)),
            dma((M, J)), dma((M, J)), dma((M, K)), dma((M, K)),
            dma((K, C)), dma((N,)), dma((N,)), dma((K, C)),
        ],
        compiler_params=pltpu.CompilerParams(collective_id=0, has_side_effects=True),
        name="crps_step",
    )(fields, observed, lat_weight[None, :], var_weight[None, :], weight, bias[None, :], gain[None, :])
    return gf, gw, gg.reshape(D), gb.reshape(V), loss.reshape(())


def solution(mesh):
    return jax.shard_map(
        shards,
        mesh=mesh,
        in_specs=(P("member", "grid", None), P(None, "grid"), P("grid"), P(), P(), P(), P()),
        out_specs=(P("member", "grid", None), P(), P(), P(), P()),
        check_vma=False,
    )
```

```python
import functools

import jax
import jax.numpy as jnp
from jax import lax
from jax.experimental import pallas as pl
from jax.experimental.pallas import tpu as pltpu
from jax.sharding import PartitionSpec as P

soft_square = 0.01
norm_epsilon = 1e-05
LANES = 128
ROW_CHUNKS = 4
POINT_BLOCK = 128
NORM_ROWS = 64
f32 = jnp.float32
bf16 = jnp.bfloat16
MESH_ID = pl.DeviceIdType.MESH


def plan(G, M, V, D):
    K = ROW_CHUNKS
    offs = [int(V * k / K / 16 + 0.5) * 16 for k in range(K)] + [V]
    rows = [offs[k + 1] - offs[k] for k in range(K)]
    extra = -(-(rows[-1] + 2) // 8) * 8
    blocks = rows[:-1] + [extra]
    C = D // LANES // 2
    per = G // 2 // K
    S = (M * per) // C
    assert G % (2 * K) == 0 and D % (2 * LANES) == 0 and (M * per) % C == 0 and S >= 1
    return K, offs, rows, blocks, C, per, S


def to_column(row, size):
    r = lax.broadcasted_iota(jnp.int32, (size, row.shape[1]), 0)
    c = lax.broadcasted_iota(jnp.int32, (size, row.shape[1]), 1)
    return jnp.sum(jnp.where(r == c, row, 0.0), axis=1, keepdims=True)


def body(G, M, fields, obs, lat, vw, w, bias, gain,
         gf, gw, gg, gb, loss,
         x, unit, normed, inv, outb, wp, gp, pred, others, lat_own, lat_sib, lat_all,
         part, sib, rs, ag_src, ag, lossb,
         in_sem, out_sem, lat_pair, lat_send, lat_recv, ps, pr, sib_send, sib_recv,
         rs_send, rs_recv, ag_send, ag_recv, fw_send, fw_recv):
    V, PTS = obs.shape
    D = w.shape[1]
    VP = wp.shape[0]
    H = G // 2
    N = H * M
    K, offs, rows, blocks, C, per, S = plan(G, M, V, D)
    ends = [-(-hi // 8) * 8 for hi in offs[1:]]
    J = PTS // POINT_BLOCK
    g = lax.axis_index("grid")
    m = lax.axis_index("member")
    q = lax.rem(g, 2)
    h = g // 2
    me = m * H + h
    my_k = lax.rem(h, K)
    my_cf = m * per + h // K
    my_c = my_cf // S
    mine = q * C
    theirs = (1 - q) * C
    sibling = {"grid": g + 1 - 2 * q, "member": m}

    def device(t):
        return {"grid": lax.rem(t, H) * 2 + q, "member": t // H}

    barrier = pltpu.get_barrier_semaphore()
    pl.semaphore_signal(barrier, inc=1, device_id=sibling, device_id_type=MESH_ID)

    @pl.loop(1, N)
    def _(i):
        pl.semaphore_signal(barrier, inc=1, device_id=device(lax.rem(me + i, N)), device_id_type=MESH_ID)

    def load(j):
        at = pl.ds(pl.multiple_of(j * POINT_BLOCK, POINT_BLOCK), POINT_BLOCK)
        return pltpu.make_async_copy(fields.at[0, at], x.at[at], in_sem.at[j])

    for j in range(J):
        load(j).start()
    wp[...] = jnp.zeros(wp.shape, bf16)
    wp[0:V, :] = w[...]
    gp[...] = jnp.zeros(gp.shape, bf16)
    lat_own[...] = jnp.full(lat_own.shape, jnp.sum(lat[...]), f32)
    bias_col = to_column(bias[...], VP)
    vw_col = to_column(vw[...], VP)
    gain_row = gain[...]

    def lat_sibling():
        return pltpu.make_async_remote_copy(
            lat_own, lat_sib, lat_pair.at[0], lat_pair.at[1], device_id=sibling, device_id_type=MESH_ID)

    def lat_copy(i):
        return pltpu.make_async_remote_copy(
            lat_all.at[h], lat_all.at[h], lat_send.at[i], lat_recv.at[h],
            device_id={"grid": lax.rem(h + i, H) * 2 + q, "member": m}, device_id_type=MESH_ID)

    def pred_copy(i, k):
        return pltpu.make_async_remote_copy(
            pred.at[offs[k]:ends[k]], others.at[i, offs[k]:ends[k]], ps.at[i, k], pr.at[i, k],
            device_id={"grid": g, "member": lax.rem(m + i, M)}, device_id_type=MESH_ID)

    def points(j):
        return pl.ds(pl.multiple_of(j * POINT_BLOCK, POINT_BLOCK), POINT_BLOCK)

    @pl.loop(0, J)
    def _(j):
        load(j).wait()
        for b in range(POINT_BLOCK // NORM_ROWS):
            at = pl.ds(pl.multiple_of(j * POINT_BLOCK + b * NORM_ROWS, NORM_ROWS), NORM_ROWS)
            values = x[at, :].astype(f32)
            centred = values - jnp.mean(values, axis=-1, keepdims=True)
            istd = lax.rsqrt(jnp.mean(centred * centred, axis=-1, keepdims=True) + norm_epsilon)
            u = centred * istd
            unit[at, :] = u
            inv[at, :] = istd
            normed[at, :] = (u * gain_row).astype(bf16)
        p = lax.dot_general(wp[...], normed[points(j), :], (((1,), (1,)), ((), ())),
                            preferred_element_type=f32)
        pred[:, points(j)] = p + bias_col

    pl.semaphore_wait(barrier, N)
    for k in range(K):
        for i in range(1, M):
            pred_copy(i, k).start()
    lat_sibling().start()

    lat_sibling().wait()
    lat_all[h] = lat_own[...] + lat_sib[...]

    @pl.loop(1, H)
    def _(i):
        lat_copy(i).start()

    def lat_all_wait():
        @pl.loop(1, H)
        def _(i):
            src = lax.rem(h + i, H)
            pltpu.make_async_copy(lat_own, lat_all.at[src], lat_recv.at[src]).wait()

    scale_pair = 1.0 / (M * (M - 1))
    lossb[...] = jnp.zeros(lossb.shape, f32)
    ones = jnp.ones((8, PTS), bf16)

    def unit_owner(k, c):
        cf = c * S
        return cf // per, (cf % per) * K + k

    def sib_copy(k):
        B = blocks[k]
        return pltpu.make_async_remote_copy(
            part.at[k, pl.ds(theirs, C), 0:B], sib.at[k, :, 0:B], sib_send.at[k], sib_recv.at[k],
            device_id=sibling, device_id_type=MESH_ID)

    def rs_copy(k, c):
        om, oh = unit_owner(k, c)
        return pltpu.make_async_remote_copy(
            part.at[k, mine + c, 0:blocks[k]], rs.at[me, 0:blocks[k]], rs_send.at[k, c], rs_recv.at[me],
            device_id={"grid": oh * 2 + q, "member": om}, device_id_type=MESH_ID)

    def not_mine(k, c):
        om, oh = unit_owner(k, c)
        return jnp.logical_or(m != om, h != oh)

    for k in range(K):
        for i in range(1, M):
            pred_copy(i, k).wait_recv()
        lo, hi, R = offs[k], offs[k + 1], rows[k]
        own = pred[lo:hi, :]
        e = own - obs[lo:hi, :].astype(f32)
        sq = e * e + soft_square
        r = lax.rsqrt(sq)
        grad = e * r * (1.0 / M)
        crps = sq * r * (1.0 / M)
        for i in range(1, M):
            e = own - others[i, lo:hi, :]
            sq = e * e + soft_square
            r = lax.rsqrt(sq)
            grad = grad - e * r * scale_pair
            crps = crps - sq * r * (0.5 * scale_pair)
        wg = vw_col[lo:hi, :] * lat[...]
        gk = (wg * grad).astype(bf16)
        lossb[...] += jnp.sum(wg * crps, axis=0, keepdims=True)
        gp[lo:hi, :] = gk
        gwk = jnp.dot(gk, normed[...], preferred_element_type=f32)
        if k == K - 1:
            gbp = lax.dot_general(ones, gp[...], (((1,), (1,)), ((), ())), preferred_element_type=f32)
            lane = jnp.zeros((1, LANES), f32)
            for j in range(PTS // LANES):
                lane = lane + lossb[:, j * LANES:(j + 1) * LANES]
        for c in range(2 * C):
            part[k, c, 0:R] = gwk[:, c * LANES:(c + 1) * LANES]
            if k == K - 1:
                part[k, c, R:R + 1] = gbp[0:1, :]
                part[k, c, R + 1:R + 2] = lane
                if blocks[k] > R + 2:
                    part[k, c, R + 2:blocks[k]] = jnp.zeros((blocks[k] - R - 2, LANES), f32)
        sib_copy(k).start()
        sib_copy(k).wait_recv()
        for c in range(C):
            part[k, mine + c, 0:blocks[k]] += sib[k, c, 0:blocks[k]]

            @pl.when(not_mine(k, c))
            def _(k=k, c=c):
                rs_copy(k, c).start()

    lat_all_wait()
    lat_total = jnp.sum(lat_all[...], axis=0)[0:1, 0:1]
    factor = (PTS * G) / lat_total

    def ag_copy(k, i):
        B = blocks[k]
        return pltpu.make_async_remote_copy(
            ag_src.at[0:B], ag.at[k, mine + my_c, 0:B], ag_send.at[i], ag_recv.at[k, my_c],
            device_id=device(lax.rem(me + i, N)), device_id_type=MESH_ID)

    is_owner = lax.rem(my_cf, S) == 0

    def reduce_and_spread(k):
        B = blocks[k]

        @pl.when(jnp.logical_and(is_owner, my_k == k))
        def _():
            def add(i, acc):
                src = lax.rem(me + i, N)
                pltpu.make_async_copy(part.at[k, 0, 0:B], rs.at[src, 0:B], rs_recv.at[src]).wait()
                return acc + rs[src, 0:B]

            acc = lax.fori_loop(1, N, add, part[k, mine + my_c, 0:B]) * factor
            ag_src[0:B] = acc
            ag[k, mine + my_c, 0:B] = acc

            @pl.loop(1, N)
            def _(i):
                ag_copy(k, i).start()

    def out_copy(j):
        return pltpu.make_async_copy(outb.at[points(j)], gf.at[0, points(j)], out_sem.at[j])

    def grad_block(j):
        gn = lax.dot_general(gp[:, points(j)], wp[...], (((0,), (0,)), ((), ())),
                             preferred_element_type=f32)
        gu = gn * gain_row
        u = unit[points(j), :]
        one = jnp.mean(gu, axis=-1, keepdims=True)
        two = jnp.mean(gu * u, axis=-1, keepdims=True)
        outb[points(j), :] = ((factor * inv[points(j), :]) * (gu - one - u * two)).astype(bf16)
        out_copy(j).start()

    for k in range(K - 2):
        reduce_and_spread(k)
    pl.loop(0, J // 2)(grad_block)
    for k in range(K - 2, K):
        reduce_and_spread(k)
    pl.loop(J // 2, J)(grad_block)

    def fw_copy(k, c):
        B = blocks[k]
        return pltpu.make_async_remote_copy(
            ag.at[k, mine + c, 0:B], ag.at[k, mine + c, 0:B], fw_send.at[k, c], fw_recv.at[k, c],
            device_id=sibling, device_id_type=MESH_ID)

    for k in range(K):
        for c in range(C):
            @pl.when(not_mine(k, c))
            def _(k=k, c=c):
                B = blocks[k]
                pltpu.make_async_copy(part.at[k, 0, 0:B], ag.at[k, mine + c, 0:B], ag_recv.at[k, c]).wait()
            fw_copy(k, c).start()
    gg_sum = [jnp.zeros((1, LANES), f32) for c in range(2 * C)]
    for k in range(K):
        lo, hi, R = offs[k], offs[k + 1], rows[k]
        for c in range(C):
            B = blocks[k]
            pltpu.make_async_copy(part.at[k, 0, 0:B], ag.at[k, theirs + c, 0:B], fw_recv.at[k, c]).wait()
        for c in range(2 * C):
            cols = slice(c * LANES, (c + 1) * LANES)
            blk = ag[k, c, 0:R]
            gw[lo:hi, cols] = blk
            gg_sum[c] = gg_sum[c] + jnp.sum(blk * w[lo:hi, cols].astype(f32), axis=0, keepdims=True)
    for c in range(2 * C):
        cols = slice(c * LANES, (c + 1) * LANES)
        gg[:, cols] = gg_sum[c] / gain_row[:, cols]
    last = rows[-1]
    gb[...] = ag[K - 1, 0, last:last + 1][:, 0:V]
    total = jnp.sum(ag[K - 1, 0, last + 1:last + 2], axis=1, keepdims=True)
    loss[...] = total / (factor * V * lat_total)

    @pl.loop(1, H)
    def _(i):
        lat_copy(i).wait_send()

    for k in range(K):
        for i in range(1, M):
            pred_copy(i, k).wait_send()
        sib_copy(k).wait_send()
        for c in range(C):
            fw_copy(k, c).wait_send()
        for c in range(C):
            @pl.when(not_mine(k, c))
            def _(k=k, c=c):
                rs_copy(k, c).wait_send()

        @pl.when(jnp.logical_and(is_owner, my_k == k))
        def _(k=k):
            @pl.loop(1, N)
            def _(i):
                ag_copy(k, i).wait_send()

    @pl.loop(0, J)
    def _(j):
        out_copy(j).wait()


def shards(fields, observed, lat_weight, var_weight, weight, bias, gain):
    G = lax.axis_size("grid")
    M = lax.axis_size("member")
    H = G // 2
    N = H * M
    V, PTS = observed.shape
    D = weight.shape[1]
    VP = -(-V // LANES) * LANES
    assert fields.shape[0] == 1 and PTS % POINT_BLOCK == 0 and VP == LANES
    K, offs, rows, blocks, C, per, S = plan(G, M, V, D)
    B = max(blocks)
    J = PTS // POINT_BLOCK
    vmem = pl.BlockSpec(memory_space=pltpu.VMEM)
    hbm = pl.BlockSpec(memory_space=pl.ANY)
    dma = pltpu.SemaphoreType.DMA
    gf, gw, gg, gb, loss = pl.pallas_call(
        functools.partial(body, G, M),
        out_shape=(
            jax.ShapeDtypeStruct(fields.shape, bf16),
            jax.ShapeDtypeStruct((V, D), f32),
            jax.ShapeDtypeStruct((1, D), f32),
            jax.ShapeDtypeStruct((1, V), f32),
            jax.ShapeDtypeStruct((1, 1), f32),
        ),
        in_specs=[hbm] + [vmem] * 6,
        out_specs=(hbm, vmem, vmem, vmem, vmem),
        scratch_shapes=[
            pltpu.VMEM((PTS, D), bf16),
            pltpu.VMEM((PTS, D), f32),
            pltpu.VMEM((PTS, D), bf16),
            pltpu.VMEM((PTS, 1), f32),
            pltpu.VMEM((PTS, D), bf16),
            pltpu.VMEM((VP, D), bf16),
            pltpu.VMEM((VP, PTS), bf16),
            pltpu.VMEM((VP, PTS), f32),
            pltpu.VMEM((M, VP, PTS), f32),
            pltpu.VMEM((8, LANES), f32),
            pltpu.VMEM((8, LANES), f32),
            pltpu.VMEM((H, 8, LANES), f32),
            pltpu.VMEM((K, 2 * C, B, LANES), f32),
            pltpu.VMEM((K, C, B, LANES), f32),
            pltpu.VMEM((N, B, LANES), f32),
            pltpu.VMEM((B, LANES), f32),
            pltpu.VMEM((K, 2 * C, B, LANES), f32),
            pltpu.VMEM((1, PTS), f32),
            dma((J,)), dma((J,)), dma((2,)), dma((H,)), dma((H,)),
            dma((M, K)), dma((M, K)), dma((K,)), dma((K,)),
            dma((K, C)), dma((N,)), dma((N,)), dma((K, C)), dma((K, C)), dma((K, C)),
        ],
        compiler_params=pltpu.CompilerParams(collective_id=0, has_side_effects=True),
        name="crps_step",
    )(fields, observed, lat_weight[None, :], var_weight[None, :], weight, bias[None, :], gain[None, :])
    return gf, gw, gg.reshape(D), gb.reshape(V), loss.reshape(())


def solution(mesh):
    return jax.shard_map(
        shards,
        mesh=mesh,
        in_specs=(P("member", "grid", None), P(None, "grid"), P("grid"), P(), P(), P(), P()),
        out_specs=(P("member", "grid", None), P(), P(), P(), P()),
        check_vma=False,
    )
```

```python
import functools

import jax
import jax.numpy as jnp
from jax import lax
from jax.experimental import pallas as pl
from jax.experimental.pallas import tpu as pltpu
from jax.sharding import PartitionSpec as P

soft_square = 0.01
norm_epsilon = 1e-05
LANES = 128
ROW_CHUNKS = 4
POINT_BLOCK = 128
NORM_ROWS = 64
f32 = jnp.float32
bf16 = jnp.bfloat16
MESH_ID = pl.DeviceIdType.MESH


def plan(G, M, V, D):
    K = ROW_CHUNKS
    offs = [int(V * k / K / 16 + 0.5) * 16 for k in range(K)] + [V]
    rows = [offs[k + 1] - offs[k] for k in range(K)]
    extra = -(-(rows[-1] + 2) // 8) * 8
    blocks = rows[:-1] + [extra]
    C = D // LANES // 2
    per = G // 2 // K
    S = (M * per) // C
    assert G % (2 * K) == 0 and D % (2 * LANES) == 0 and (M * per) % C == 0 and S >= 1
    return K, offs, rows, blocks, C, per, S


def to_column(row, size):
    r = lax.broadcasted_iota(jnp.int32, (size, row.shape[1]), 0)
    c = lax.broadcasted_iota(jnp.int32, (size, row.shape[1]), 1)
    return jnp.sum(jnp.where(r == c, row, 0.0), axis=1, keepdims=True)


def body(G, M, fields, obs, lat, vw, w, bias, gain,
         gf, gw, gg, gb, loss,
         x, unit, normed, inv, wp, gp, pred, others, lat_own, lat_sib, lat_all,
         part, sib, rs, ag_src, ag, lossb,
         in_sem, lat_pair, lat_send, lat_recv, ps, pr, sib_send, sib_recv,
         rs_send, rs_recv, ag_send, ag_recv, fw_send, fw_recv):
    V, PTS = obs.shape
    D = w.shape[1]
    VP = wp.shape[0]
    H = G // 2
    N = H * M
    K, offs, rows, blocks, C, per, S = plan(G, M, V, D)
    ends = [-(-hi // 8) * 8 for hi in offs[1:]]
    J = PTS // POINT_BLOCK
    g = lax.axis_index("grid")
    m = lax.axis_index("member")
    q = lax.rem(g, 2)
    h = g // 2
    me = m * H + h
    my_k = lax.rem(h, K)
    my_cf = m * per + h // K
    my_c = my_cf // S
    mine = q * C
    theirs = (1 - q) * C
    sibling = {"grid": g + 1 - 2 * q, "member": m}

    def device(t):
        return {"grid": lax.rem(t, H) * 2 + q, "member": t // H}

    barrier = pltpu.get_barrier_semaphore()
    pl.semaphore_signal(barrier, inc=1, device_id=sibling, device_id_type=MESH_ID)

    @pl.loop(1, N)
    def _(i):
        pl.semaphore_signal(barrier, inc=1, device_id=device(lax.rem(me + i, N)), device_id_type=MESH_ID)

    def load(j):
        at = pl.ds(pl.multiple_of(j * POINT_BLOCK, POINT_BLOCK), POINT_BLOCK)
        return pltpu.make_async_copy(fields.at[0, at], x.at[at], in_sem.at[j])

    for j in range(J):
        load(j).start()
    wp[...] = jnp.zeros(wp.shape, bf16)
    wp[0:V, :] = w[...]
    gp[...] = jnp.zeros(gp.shape, bf16)
    lat_own[...] = jnp.full(lat_own.shape, jnp.sum(lat[...]), f32)
    bias_col = to_column(bias[...], VP)
    vw_col = to_column(vw[...], VP)
    gain_row = gain[...]

    def lat_sibling():
        return pltpu.make_async_remote_copy(
            lat_own, lat_sib, lat_pair.at[0], lat_pair.at[1], device_id=sibling, device_id_type=MESH_ID)

    def lat_copy(i):
        return pltpu.make_async_remote_copy(
            lat_all.at[h], lat_all.at[h], lat_send.at[i], lat_recv.at[h],
            device_id={"grid": lax.rem(h + i, H) * 2 + q, "member": m}, device_id_type=MESH_ID)

    def pred_copy(i, k):
        return pltpu.make_async_remote_copy(
            pred.at[offs[k]:ends[k]], others.at[i, offs[k]:ends[k]], ps.at[i, k], pr.at[i, k],
            device_id={"grid": g, "member": lax.rem(m + i, M)}, device_id_type=MESH_ID)

    def points(j):
        return pl.ds(pl.multiple_of(j * POINT_BLOCK, POINT_BLOCK), POINT_BLOCK)

    @pl.loop(0, J)
    def _(j):
        load(j).wait()
        for b in range(POINT_BLOCK // NORM_ROWS):
            at = pl.ds(pl.multiple_of(j * POINT_BLOCK + b * NORM_ROWS, NORM_ROWS), NORM_ROWS)
            values = x[at, :].astype(f32)
            centred = values - jnp.mean(values, axis=-1, keepdims=True)
            istd = lax.rsqrt(jnp.mean(centred * centred, axis=-1, keepdims=True) + norm_epsilon)
            u = centred * istd
            unit[at, :] = u
            inv[at, :] = istd
            normed[at, :] = (u * gain_row).astype(bf16)
        p = lax.dot_general(wp[...], normed[points(j), :], (((1,), (1,)), ((), ())),
                            preferred_element_type=f32)
        pred[:, points(j)] = p + bias_col

    pl.semaphore_wait(barrier, N)
    for k in range(K):
        for i in range(1, M):
            pred_copy(i, k).start()
    lat_sibling().start()

    lat_sibling().wait()
    lat_all[h] = lat_own[...] + lat_sib[...]

    @pl.loop(1, H)
    def _(i):
        lat_copy(i).start()

    def lat_all_wait():
        @pl.loop(1, H)
        def _(i):
            src = lax.rem(h + i, H)
            pltpu.make_async_copy(lat_own, lat_all.at[src], lat_recv.at[src]).wait()

    scale_pair = 1.0 / (M * (M - 1))
    lossb[...] = jnp.zeros(lossb.shape, f32)
    ones = jnp.ones((8, PTS), bf16)

    def unit_owner(k, c):
        cf = c * S
        return cf // per, (cf % per) * K + k

    def sib_copy(k):
        B = blocks[k]
        return pltpu.make_async_remote_copy(
            part.at[k, pl.ds(theirs, C), 0:B], sib.at[k, :, 0:B], sib_send.at[k], sib_recv.at[k],
            device_id=sibling, device_id_type=MESH_ID)

    def rs_copy(k, c):
        om, oh = unit_owner(k, c)
        return pltpu.make_async_remote_copy(
            part.at[k, mine + c, 0:blocks[k]], rs.at[me, 0:blocks[k]], rs_send.at[k, c], rs_recv.at[me],
            device_id={"grid": oh * 2 + q, "member": om}, device_id_type=MESH_ID)

    def not_mine(k, c):
        om, oh = unit_owner(k, c)
        return jnp.logical_or(m != om, h != oh)

    for k in range(K):
        for i in range(1, M):
            pred_copy(i, k).wait_recv()
        lo, hi, R = offs[k], offs[k + 1], rows[k]
        own = pred[lo:hi, :]
        e = own - obs[lo:hi, :].astype(f32)
        sq = e * e + soft_square
        r = lax.rsqrt(sq)
        grad = e * r * (1.0 / M)
        crps = sq * r * (1.0 / M)
        for i in range(1, M):
            e = own - others[i, lo:hi, :]
            sq = e * e + soft_square
            r = lax.rsqrt(sq)
            grad = grad - e * r * scale_pair
            crps = crps - sq * r * (0.5 * scale_pair)
        wg = vw_col[lo:hi, :] * lat[...]
        gk = (wg * grad).astype(bf16)
        lossb[...] += jnp.sum(wg * crps, axis=0, keepdims=True)
        gp[lo:hi, :] = gk
        gwk = jnp.dot(gk, normed[...], preferred_element_type=f32)
        if k == K - 1:
            gbp = lax.dot_general(ones, gp[...], (((1,), (1,)), ((), ())), preferred_element_type=f32)
            lane = jnp.zeros((1, LANES), f32)
            for j in range(PTS // LANES):
                lane = lane + lossb[:, j * LANES:(j + 1) * LANES]
        for c in range(2 * C):
            part[k, c, 0:R] = gwk[:, c * LANES:(c + 1) * LANES]
            if k == K - 1:
                part[k, c, R:R + 1] = gbp[0:1, :]
                part[k, c, R + 1:R + 2] = lane
                if blocks[k] > R + 2:
                    part[k, c, R + 2:blocks[k]] = jnp.zeros((blocks[k] - R - 2, LANES), f32)
        sib_copy(k).start()
        sib_copy(k).wait_recv()
        for c in range(C):
            part[k, mine + c, 0:blocks[k]] += sib[k, c, 0:blocks[k]]

            @pl.when(not_mine(k, c))
            def _(k=k, c=c):
                rs_copy(k, c).start()

    lat_all_wait()
    lat_total = jnp.sum(lat_all[...], axis=0)[0:1, 0:1]
    factor = (PTS * G) / lat_total

    def ag_copy(k, i):
        B = blocks[k]
        return pltpu.make_async_remote_copy(
            ag_src.at[0:B], ag.at[k, mine + my_c, 0:B], ag_send.at[i], ag_recv.at[k, my_c],
            device_id=device(lax.rem(me + i, N)), device_id_type=MESH_ID)

    is_owner = lax.rem(my_cf, S) == 0

    def reduce_and_spread(k):
        B = blocks[k]

        @pl.when(jnp.logical_and(is_owner, my_k == k))
        def _():
            def add(i, acc):
                src = lax.rem(me + i, N)
                pltpu.make_async_copy(part.at[k, 0, 0:B], rs.at[src, 0:B], rs_recv.at[src]).wait()
                return acc + rs[src, 0:B]

            acc = lax.fori_loop(1, N, add, part[k, mine + my_c, 0:B]) * factor
            ag_src[0:B] = acc
            ag[k, mine + my_c, 0:B] = acc

            @pl.loop(1, N)
            def _(i):
                ag_copy(k, i).start()

    def grad_block(j):
        gn = lax.dot_general(gp[:, points(j)], wp[...], (((0,), (0,)), ((), ())),
                             preferred_element_type=f32)
        gu = gn * gain_row
        u = unit[points(j), :]
        one = jnp.mean(gu, axis=-1, keepdims=True)
        two = jnp.mean(gu * u, axis=-1, keepdims=True)
        gf[points(j), :] = ((factor * inv[points(j), :]) * (gu - one - u * two)).astype(bf16)

    for k in range(K - 2):
        reduce_and_spread(k)
    pl.loop(0, J // 2)(grad_block)
    for k in range(K - 2, K):
        reduce_and_spread(k)
    pl.loop(J // 2, J)(grad_block)

    def fw_copy(k, c):
        B = blocks[k]
        return pltpu.make_async_remote_copy(
            ag.at[k, mine + c, 0:B], ag.at[k, mine + c, 0:B], fw_send.at[k, c], fw_recv.at[k, c],
            device_id=sibling, device_id_type=MESH_ID)

    for k in range(K):
        for c in range(C):
            @pl.when(not_mine(k, c))
            def _(k=k, c=c):
                B = blocks[k]
                pltpu.make_async_copy(part.at[k, 0, 0:B], ag.at[k, mine + c, 0:B], ag_recv.at[k, c]).wait()
            fw_copy(k, c).start()
    gg_sum = [jnp.zeros((1, LANES), f32) for c in range(2 * C)]
    for k in range(K):
        lo, hi, R = offs[k], offs[k + 1], rows[k]
        for c in range(C):
            B = blocks[k]
            pltpu.make_async_copy(part.at[k, 0, 0:B], ag.at[k, theirs + c, 0:B], fw_recv.at[k, c]).wait()
        for c in range(2 * C):
            cols = slice(c * LANES, (c + 1) * LANES)
            blk = ag[k, c, 0:R]
            gw[lo:hi, cols] = blk
            gg_sum[c] = gg_sum[c] + jnp.sum(blk * w[lo:hi, cols].astype(f32), axis=0, keepdims=True)
    for c in range(2 * C):
        cols = slice(c * LANES, (c + 1) * LANES)
        gg[:, cols] = gg_sum[c] / gain_row[:, cols]
    last = rows[-1]
    gb[...] = ag[K - 1, 0, last:last + 1][:, 0:V]
    total = jnp.sum(ag[K - 1, 0, last + 1:last + 2], axis=1, keepdims=True)
    loss[...] = total / (factor * V * lat_total)

    @pl.loop(1, H)
    def _(i):
        lat_copy(i).wait_send()

    for k in range(K):
        for i in range(1, M):
            pred_copy(i, k).wait_send()
        sib_copy(k).wait_send()
        for c in range(C):
            fw_copy(k, c).wait_send()
        for c in range(C):
            @pl.when(not_mine(k, c))
            def _(k=k, c=c):
                rs_copy(k, c).wait_send()

        @pl.when(jnp.logical_and(is_owner, my_k == k))
        def _(k=k):
            @pl.loop(1, N)
            def _(i):
                ag_copy(k, i).wait_send()


def write_out(*refs):
    n = len(refs) // 2
    sem = refs[-1]
    copies = [pltpu.make_async_copy(refs[i], refs[n + i], sem.at[i]) for i in range(n)]
    for copy in copies:
        copy.start()
    for copy in copies:
        copy.wait()


def shards(fields, observed, lat_weight, var_weight, weight, bias, gain):
    G = lax.axis_size("grid")
    M = lax.axis_size("member")
    H = G // 2
    N = H * M
    V, PTS = observed.shape
    D = weight.shape[1]
    VP = -(-V // LANES) * LANES
    assert fields.shape[0] == 1 and PTS % POINT_BLOCK == 0 and VP == LANES
    K, offs, rows, blocks, C, per, S = plan(G, M, V, D)
    B = max(blocks)
    J = PTS // POINT_BLOCK
    vmem = pl.BlockSpec(memory_space=pltpu.VMEM)
    hbm = pl.BlockSpec(memory_space=pl.ANY)
    dma = pltpu.SemaphoreType.DMA
    held = pl.pallas_call(
        functools.partial(body, G, M),
        out_shape=(
            pltpu.VMEM((PTS, D), bf16),
            pltpu.VMEM((V, D), f32),
            pltpu.VMEM((1, D), f32),
            pltpu.VMEM((1, V), f32),
            pltpu.VMEM((1, 1), f32),
        ),
        in_specs=[hbm] + [vmem] * 6,
        out_specs=(vmem,) * 5,
        scratch_shapes=[
            pltpu.VMEM((PTS, D), bf16),
            pltpu.VMEM((PTS, D), f32),
            pltpu.VMEM((PTS, D), bf16),
            pltpu.VMEM((PTS, 1), f32),
            pltpu.VMEM((VP, D), bf16),
            pltpu.VMEM((VP, PTS), bf16),
            pltpu.VMEM((VP, PTS), f32),
            pltpu.VMEM((M, VP, PTS), f32),
            pltpu.VMEM((8, LANES), f32),
            pltpu.VMEM((8, LANES), f32),
            pltpu.VMEM((H, 8, LANES), f32),
            pltpu.VMEM((K, 2 * C, B, LANES), f32),
            pltpu.VMEM((K, C, B, LANES), f32),
            pltpu.VMEM((N, B, LANES), f32),
            pltpu.VMEM((B, LANES), f32),
            pltpu.VMEM((K, 2 * C, B, LANES), f32),
            pltpu.VMEM((1, PTS), f32),
            dma((J,)), dma((2,)), dma((H,)), dma((H,)),
            dma((M, K)), dma((M, K)), dma((K,)), dma((K,)),
            dma((K, C)), dma((N,)), dma((N,)), dma((K, C)), dma((K, C)), dma((K, C)),
        ],
        compiler_params=pltpu.CompilerParams(collective_id=0, has_side_effects=True),
        name="crps_step",
    )(fields, observed, lat_weight[None, :], var_weight[None, :], weight, bias[None, :], gain[None, :])
    gf, gw, gg, gb, loss = pl.pallas_call(
        write_out,
        out_shape=tuple(jax.ShapeDtypeStruct(a.shape, a.dtype) for a in held),
        in_specs=[vmem] * 5,
        out_specs=(hbm,) * 5,
        scratch_shapes=[dma((5,))],
        name="write_out",
    )(*[pltpu.with_memory_space_constraint(a, pltpu.VMEM) for a in held])
    return gf.reshape(fields.shape), gw, gg.reshape(D), gb.reshape(V), loss.reshape(())


def solution(mesh):
    return jax.shard_map(
        shards,
        mesh=mesh,
        in_specs=(P("member", "grid", None), P(None, "grid"), P("grid"), P(), P(), P(), P()),
        out_specs=(P("member", "grid", None), P(), P(), P(), P()),
        check_vma=False,
    )
```

```python
import functools

import jax
import jax.numpy as jnp
from jax import lax
from jax.experimental import pallas as pl
from jax.experimental.pallas import tpu as pltpu
from jax.sharding import PartitionSpec as P

soft_square = 0.01
norm_epsilon = 1e-05
LANES = 128
ROW_CHUNKS = 4
POINT_BLOCK = 128
NORM_ROWS = 64
f32 = jnp.float32
bf16 = jnp.bfloat16
MESH_ID = pl.DeviceIdType.MESH


def plan(G, M, V, D):
    K = ROW_CHUNKS
    offs = [-(-V * k // (16 * K)) * 16 for k in range(K)] + [V]
    rows = [offs[k + 1] - offs[k] for k in range(K)]
    extra = -(-(rows[-1] + 2) // 8) * 8
    blocks = rows[:-1] + [extra]
    C = D // LANES // 2
    per = G // 2 // K
    S = (M * per) // C
    assert G % (2 * K) == 0 and D % (2 * LANES) == 0 and (M * per) % C == 0 and S >= 1
    return K, offs, rows, blocks, C, per, S


def to_column(row, size):
    r = lax.broadcasted_iota(jnp.int32, (size, row.shape[1]), 0)
    c = lax.broadcasted_iota(jnp.int32, (size, row.shape[1]), 1)
    return jnp.sum(jnp.where(r == c, row, 0.0), axis=1, keepdims=True)


def body(G, M, fields, obs, lat, vw, w, bias, gain,
         gf, gw, gg, gb, loss,
         x, unit, normed, inv, wp, gp, pred, others, lat_own, lat_sib, lat_all,
         part, sib, rs, ag_src, ag, lossb,
         in_sem, lat_pair, lat_send, lat_recv, ps, pr, sib_send, sib_recv,
         rs_send, rs_recv, ag_send, ag_recv, fw_send, fw_recv):
    V, PTS = obs.shape
    D = w.shape[1]
    VP = wp.shape[0]
    H = G // 2
    N = H * M
    K, offs, rows, blocks, C, per, S = plan(G, M, V, D)
    ends = [-(-hi // 8) * 8 for hi in offs[1:]]
    J = PTS // POINT_BLOCK
    g = lax.axis_index("grid")
    m = lax.axis_index("member")
    q = lax.rem(g, 2)
    h = g // 2
    me = m * H + h
    my_k = lax.rem(h, K)
    my_cf = m * per + h // K
    my_c = my_cf // S
    mine = q * C
    theirs = (1 - q) * C
    sibling = {"grid": g + 1 - 2 * q, "member": m}

    def device(t):
        return {"grid": lax.rem(t, H) * 2 + q, "member": t // H}

    barrier = pltpu.get_barrier_semaphore()
    pl.semaphore_signal(barrier, inc=1, device_id=sibling, device_id_type=MESH_ID)

    @pl.loop(1, N)
    def _(i):
        pl.semaphore_signal(barrier, inc=1, device_id=device(lax.rem(me + i, N)), device_id_type=MESH_ID)

    def load(j):
        at = pl.ds(pl.multiple_of(j * POINT_BLOCK, POINT_BLOCK), POINT_BLOCK)
        return pltpu.make_async_copy(fields.at[0, at], x.at[at], in_sem.at[j])

    for j in range(J):
        load(j).start()
    wp[...] = jnp.zeros(wp.shape, bf16)
    wp[0:V, :] = w[...]
    gp[...] = jnp.zeros(gp.shape, bf16)
    lat_own[...] = jnp.full(lat_own.shape, jnp.sum(lat[...]), f32)
    bias_col = to_column(bias[...], VP)
    vw_col = to_column(vw[...], VP)
    gain_row = gain[...]

    def lat_sibling():
        return pltpu.make_async_remote_copy(
            lat_own, lat_sib, lat_pair.at[0], lat_pair.at[1], device_id=sibling, device_id_type=MESH_ID)

    def lat_copy(i):
        return pltpu.make_async_remote_copy(
            lat_all.at[h], lat_all.at[h], lat_send.at[i], lat_recv.at[h],
            device_id={"grid": lax.rem(h + i, H) * 2 + q, "member": m}, device_id_type=MESH_ID)

    def pred_copy(i, k):
        return pltpu.make_async_remote_copy(
            pred.at[offs[k]:ends[k]], others.at[i, offs[k]:ends[k]], ps.at[i, k], pr.at[i, k],
            device_id={"grid": g, "member": lax.rem(m + i, M)}, device_id_type=MESH_ID)

    def points(j):
        return pl.ds(pl.multiple_of(j * POINT_BLOCK, POINT_BLOCK), POINT_BLOCK)

    @pl.loop(0, J)
    def _(j):
        load(j).wait()
        for b in range(POINT_BLOCK // NORM_ROWS):
            at = pl.ds(pl.multiple_of(j * POINT_BLOCK + b * NORM_ROWS, NORM_ROWS), NORM_ROWS)
            values = x[at, :].astype(f32)
            centred = values - jnp.mean(values, axis=-1, keepdims=True)
            istd = lax.rsqrt(jnp.mean(centred * centred, axis=-1, keepdims=True) + norm_epsilon)
            u = centred * istd
            unit[at, :] = u
            inv[at, :] = istd
            normed[at, :] = (u * gain_row).astype(bf16)
        p = lax.dot_general(wp[...], normed[points(j), :], (((1,), (1,)), ((), ())),
                            preferred_element_type=f32)
        pred[:, points(j)] = p + bias_col

    pl.semaphore_wait(barrier, N)
    for k in range(K):
        for i in range(1, M):
            pred_copy(i, k).start()
    lat_sibling().start()

    lat_sibling().wait()
    lat_all[h] = lat_own[...] + lat_sib[...]

    @pl.loop(1, H)
    def _(i):
        lat_copy(i).start()

    def lat_all_wait():
        @pl.loop(1, H)
        def _(i):
            src = lax.rem(h + i, H)
            pltpu.make_async_copy(lat_own, lat_all.at[src], lat_recv.at[src]).wait()

    scale_pair = 1.0 / (M * (M - 1))
    lossb[...] = jnp.zeros(lossb.shape, f32)
    ones = jnp.ones((8, PTS), bf16)

    def unit_owner(k, c):
        cf = c * S
        return cf // per, (cf % per) * K + k

    def sib_copy(k):
        B = blocks[k]
        return pltpu.make_async_remote_copy(
            part.at[k, pl.ds(theirs, C), 0:B], sib.at[k, :, 0:B], sib_send.at[k], sib_recv.at[k],
            device_id=sibling, device_id_type=MESH_ID)

    def rs_copy(k, c):
        om, oh = unit_owner(k, c)
        return pltpu.make_async_remote_copy(
            part.at[k, mine + c, 0:blocks[k]], rs.at[me, 0:blocks[k]], rs_send.at[k, c], rs_recv.at[me],
            device_id={"grid": oh * 2 + q, "member": om}, device_id_type=MESH_ID)

    def not_mine(k, c):
        om, oh = unit_owner(k, c)
        return jnp.logical_or(m != om, h != oh)

    for k in range(K):
        for i in range(1, M):
            pred_copy(i, k).wait_recv()
        lo, hi, R = offs[k], offs[k + 1], rows[k]
        own = pred[lo:hi, :]
        e = own - obs[lo:hi, :].astype(f32)
        sq = e * e + soft_square
        r = lax.rsqrt(sq)
        grad = e * r * (1.0 / M)
        crps = sq * r * (1.0 / M)
        for i in range(1, M):
            e = own - others[i, lo:hi, :]
            sq = e * e + soft_square
            r = lax.rsqrt(sq)
            grad = grad - e * r * scale_pair
            crps = crps - sq * r * (0.5 * scale_pair)
        wg = vw_col[lo:hi, :] * lat[...]
        gk = (wg * grad).astype(bf16)
        lossb[...] += jnp.sum(wg * crps, axis=0, keepdims=True)
        gp[lo:hi, :] = gk
        gwk = jnp.dot(gk, normed[...], preferred_element_type=f32)
        if k == K - 1:
            gbp = lax.dot_general(ones, gp[...], (((1,), (1,)), ((), ())), preferred_element_type=f32)
            lane = jnp.zeros((1, LANES), f32)
            for j in range(PTS // LANES):
                lane = lane + lossb[:, j * LANES:(j + 1) * LANES]
        for c in range(2 * C):
            part[k, c, 0:R] = gwk[:, c * LANES:(c + 1) * LANES]
            if k == K - 1:
                part[k, c, R:R + 1] = gbp[0:1, :]
                part[k, c, R + 1:R + 2] = lane
                if blocks[k] > R + 2:
                    part[k, c, R + 2:blocks[k]] = jnp.zeros((blocks[k] - R - 2, LANES), f32)
        sib_copy(k).start()
        sib_copy(k).wait_recv()
        for c in range(C):
            part[k, mine + c, 0:blocks[k]] += sib[k, c, 0:blocks[k]]

            @pl.when(not_mine(k, c))
            def _(k=k, c=c):
                rs_copy(k, c).start()

    lat_all_wait()
    lat_total = jnp.sum(lat_all[...], axis=0)[0:1, 0:1]
    factor = (PTS * G) / lat_total

    def ag_copy(k, i):
        B = blocks[k]
        return pltpu.make_async_remote_copy(
            ag_src.at[0:B], ag.at[k, mine + my_c, 0:B], ag_send.at[i], ag_recv.at[k, my_c],
            device_id=device(lax.rem(me + i, N)), device_id_type=MESH_ID)

    is_owner = lax.rem(my_cf, S) == 0

    def reduce_and_spread(k):
        B = blocks[k]

        @pl.when(jnp.logical_and(is_owner, my_k == k))
        def _():
            def add(i, acc):
                src = lax.rem(me + i, N)
                pltpu.make_async_copy(part.at[k, 0, 0:B], rs.at[src, 0:B], rs_recv.at[src]).wait()
                return acc + rs[src, 0:B]

            acc = lax.fori_loop(1, N, add, part[k, mine + my_c, 0:B]) * factor
            ag_src[0:B] = acc
            ag[k, mine + my_c, 0:B] = acc

            @pl.loop(1, N)
            def _(i):
                ag_copy(k, i).start()

    def grad_block(j):
        gn = lax.dot_general(gp[:, points(j)], wp[...], (((0,), (0,)), ((), ())),
                             preferred_element_type=f32)
        gu = gn * gain_row
        u = unit[points(j), :]
        one = jnp.mean(gu, axis=-1, keepdims=True)
        two = jnp.mean(gu * u, axis=-1, keepdims=True)
        gf[points(j), :] = ((factor * inv[points(j), :]) * (gu - one - u * two)).astype(bf16)

    for k in range(K - 2):
        reduce_and_spread(k)
    pl.loop(0, J // 2)(grad_block)
    for k in range(K - 2, K):
        reduce_and_spread(k)
    pl.loop(J // 2, J)(grad_block)

    def fw_copy(k, c):
        B = blocks[k]
        return pltpu.make_async_remote_copy(
            ag.at[k, mine + c, 0:B], ag.at[k, mine + c, 0:B], fw_send.at[k, c], fw_recv.at[k, c],
            device_id=sibling, device_id_type=MESH_ID)

    for k in range(K):
        for c in range(C):
            @pl.when(not_mine(k, c))
            def _(k=k, c=c):
                B = blocks[k]
                pltpu.make_async_copy(part.at[k, 0, 0:B], ag.at[k, mine + c, 0:B], ag_recv.at[k, c]).wait()
            fw_copy(k, c).start()
    gg_sum = [jnp.zeros((1, LANES), f32) for c in range(2 * C)]
    for k in range(K):
        lo, hi, R = offs[k], offs[k + 1], rows[k]
        for c in range(C):
            B = blocks[k]
            pltpu.make_async_copy(part.at[k, 0, 0:B], ag.at[k, theirs + c, 0:B], fw_recv.at[k, c]).wait()
        for c in range(2 * C):
            cols = slice(c * LANES, (c + 1) * LANES)
            blk = ag[k, c, 0:R]
            gw[lo:hi, cols] = blk
            gg_sum[c] = gg_sum[c] + jnp.sum(blk * w[lo:hi, cols].astype(f32), axis=0, keepdims=True)
    for c in range(2 * C):
        cols = slice(c * LANES, (c + 1) * LANES)
        gg[:, cols] = gg_sum[c] / gain_row[:, cols]
    last = rows[-1]
    gb[...] = ag[K - 1, 0, last:last + 1][:, 0:V]
    total = jnp.sum(ag[K - 1, 0, last + 1:last + 2], axis=1, keepdims=True)
    loss[...] = total / (factor * V * lat_total)

    @pl.loop(1, H)
    def _(i):
        lat_copy(i).wait_send()

    for k in range(K):
        for i in range(1, M):
            pred_copy(i, k).wait_send()
        sib_copy(k).wait_send()
        for c in range(C):
            fw_copy(k, c).wait_send()
        for c in range(C):
            @pl.when(not_mine(k, c))
            def _(k=k, c=c):
                rs_copy(k, c).wait_send()

        @pl.when(jnp.logical_and(is_owner, my_k == k))
        def _(k=k):
            @pl.loop(1, N)
            def _(i):
                ag_copy(k, i).wait_send()


def write_out(*refs):
    n = len(refs) // 2
    sem = refs[-1]
    copies = [pltpu.make_async_copy(refs[i], refs[n + i], sem.at[i]) for i in range(n)]
    for copy in copies:
        copy.start()
    for copy in copies:
        copy.wait()


def shards(fields, observed, lat_weight, var_weight, weight, bias, gain):
    G = lax.axis_size("grid")
    M = lax.axis_size("member")
    H = G // 2
    N = H * M
    V, PTS = observed.shape
    D = weight.shape[1]
    VP = -(-V // LANES) * LANES
    assert fields.shape[0] == 1 and PTS % POINT_BLOCK == 0 and VP == LANES
    K, offs, rows, blocks, C, per, S = plan(G, M, V, D)
    B = max(blocks)
    J = PTS // POINT_BLOCK
    vmem = pl.BlockSpec(memory_space=pltpu.VMEM)
    hbm = pl.BlockSpec(memory_space=pl.ANY)
    dma = pltpu.SemaphoreType.DMA
    held = pl.pallas_call(
        functools.partial(body, G, M),
        out_shape=(
            pltpu.VMEM((PTS, D), bf16),
            pltpu.VMEM((V, D), f32),
            pltpu.VMEM((1, D), f32),
            pltpu.VMEM((1, V), f32),
            pltpu.VMEM((1, 1), f32),
        ),
        in_specs=[hbm] + [vmem] * 6,
        out_specs=(vmem,) * 5,
        scratch_shapes=[
            pltpu.VMEM((PTS, D), bf16),
            pltpu.VMEM((PTS, D), f32),
            pltpu.VMEM((PTS, D), bf16),
            pltpu.VMEM((PTS, 1), f32),
            pltpu.VMEM((VP, D), bf16),
            pltpu.VMEM((VP, PTS), bf16),
            pltpu.VMEM((VP, PTS), f32),
            pltpu.VMEM((M, VP, PTS), f32),
            pltpu.VMEM((8, LANES), f32),
            pltpu.VMEM((8, LANES), f32),
            pltpu.VMEM((H, 8, LANES), f32),
            pltpu.VMEM((K, 2 * C, B, LANES), f32),
            pltpu.VMEM((K, C, B, LANES), f32),
            pltpu.VMEM((N, B, LANES), f32),
            pltpu.VMEM((B, LANES), f32),
            pltpu.VMEM((K, 2 * C, B, LANES), f32),
            pltpu.VMEM((1, PTS), f32),
            dma((J,)), dma((2,)), dma((H,)), dma((H,)),
            dma((M, K)), dma((M, K)), dma((K,)), dma((K,)),
            dma((K, C)), dma((N,)), dma((N,)), dma((K, C)), dma((K, C)), dma((K, C)),
        ],
        compiler_params=pltpu.CompilerParams(collective_id=0, has_side_effects=True),
        name="crps_step",
    )(fields, observed, lat_weight[None, :], var_weight[None, :], weight, bias[None, :], gain[None, :])
    gf, gw, gg, gb, loss = pl.pallas_call(
        write_out,
        out_shape=tuple(jax.ShapeDtypeStruct(a.shape, a.dtype) for a in held),
        in_specs=[vmem] * 5,
        out_specs=(hbm,) * 5,
        scratch_shapes=[dma((5,))],
        name="write_out",
    )(*[pltpu.with_memory_space_constraint(a, pltpu.VMEM) for a in held])
    return gf.reshape(fields.shape), gw, gg.reshape(D), gb.reshape(V), loss.reshape(())


def solution(mesh):
    return jax.shard_map(
        shards,
        mesh=mesh,
        in_specs=(P("member", "grid", None), P(None, "grid"), P("grid"), P(), P(), P(), P()),
        out_specs=(P("member", "grid", None), P(), P(), P(), P()),
        check_vma=False,
    )
```
